32 devices in a mesh: aux: 16 (over z, y, x), ao: 2 (over core).
Axes of the slice: x: 2, y: 2, z: 4, core: 2. Of those that a mesh axis runs over, the one named last changes fastest.
Arguments:
- ints: bfloat16 [256, 768, 768], P('aux', 'ao'), may hold values from -1.25 to 1.25
- occ_coef: bfloat16 [768, 32], replicated, may hold values from -0.21875 to 0.21875
- vir_coef: bfloat16 [768, 512], P('ao'), may hold values from -0.21875 to 0.21875
- occ_energy: float32 [32], replicated, may hold values from -2 to -0.3
- vir_energy: float32 [512], replicated, may hold values from 0.3 to 3
Outputs:
- density: float32 [32, 512, 512], P('aux', 'ao')
The draws below stay inside these ranges and needn't reach their ends.
All inputs are finite; a program needn't handle non-finite values.
Results may differ from the reference program's by a relative error of at most 0.0065.
Values may be sent and summed in bfloat16 or wider, within the bound.
A program may use at most 128 MiB of HBM per device.

```python
import jax
import jax.numpy as jnp
from jax import lax

AO = 768
NVIR = 512
OCC_DEV = 2
CYCLE = 4
NOCC = 32
NAUX = 256
N_AUX = 16


def block_scale(stream_key, extent, pieces, least, top_value):
    gain, own = 1.0, jax.random.fold_in(stream_key, 6)
    for axis_at, blocks in pieces:
        heights = jnp.exp(jax.random.uniform(jax.random.fold_in(own, axis_at), (blocks,), jnp.float32, least / len(pieces), top_value / len(pieces)))
        gain = gain * jnp.repeat(heights, extent[axis_at] // blocks).reshape([-1 if axis == axis_at else 1 for axis in range(len(extent))])
    return gain


def centred(own_key, dims, width, bound, cuts=(), held_as=jnp.bfloat16):
    level = block_scale(own_key, dims, cuts, -0.22, 0.18) if cuts else 1.0
    drawn = jax.random.normal(own_key, dims, jnp.float32) * width * level
    return jnp.minimum(jnp.maximum(drawn, -bound), bound).astype(held_as)


def setup_inputs(seed: int = 0) -> dict:
    key_list = jax.random.split(jax.random.key(seed), 6)
    ints = centred(key_list[0], (NAUX, AO, AO), 0.08, 1.25, ((0, 16), (1, 2)))
    occ_coef = centred(key_list[1], (AO, NOCC), AO ** -0.5, 0.21875)
    vir_coef = centred(key_list[2], (AO, NVIR), AO ** -0.5, 0.21875, ((0, 2),))
    occ_energy = jnp.clip(jax.random.uniform(key_list[3], (NOCC,), jnp.float32, -2.0, -0.3), -2.0, -0.3)
    vir_energy = jnp.clip(jax.random.uniform(key_list[4], (NVIR,), jnp.float32, 0.3, 3.0), 0.3, 3.0)
    return {"ints": ints, "occ_coef": occ_coef, "vir_coef": vir_coef, "occ_energy": occ_energy, "vir_energy": vir_energy}


def reference(ints, occ_coef, vir_coef, occ_energy, vir_energy):
    def transform(slab):
        half_ints = jnp.dot(slab, occ_coef, preferred_element_type=jnp.float32).astype(jnp.bfloat16)
        return jnp.dot(half_ints.T, vir_coef, preferred_element_type=jnp.float32).astype(jnp.bfloat16)

    three = lax.map(transform, ints)
    offsets = jnp.arange(2 * CYCLE + 1, dtype=jnp.int32) - CYCLE
    inside = jnp.arange(OCC_DEV, dtype=jnp.int32)
    vir_pairs = vir_energy[:, None] + vir_energy[None, :]

    def one_orbital(orbital):
        block_index = orbital // OCC_DEV
        blocks = (block_index + offsets + N_AUX) % N_AUX
        partners = (blocks[:, None] * OCC_DEV + inside[None, :]).reshape(-1).astype(jnp.int32)
        partner_rows = jnp.take(three, partners, axis=1).astype(jnp.float32)
        own_rows = lax.dynamic_index_in_dim(three, orbital, 1, keepdims=False).astype(jnp.float32)
        integrals = jnp.einsum("qa,qjb->jab", own_rows, partner_rows)
        own_energy = lax.dynamic_index_in_dim(occ_energy, orbital, 0, keepdims=False)
        pair_energy = jnp.take(occ_energy, partners, axis=0)
        energy_gap = own_energy + pair_energy[:, None, None] - vir_pairs[None]
        scaled = integrals / energy_gap
        amplitude = scaled.astype(jnp.bfloat16).astype(jnp.float32)
        mixed = (2.0 * scaled - jnp.swapaxes(scaled, 1, 2)).astype(jnp.bfloat16).astype(jnp.float32)
        return jnp.einsum("jac,jbc->ab", amplitude, mixed)

    return lax.map(one_orbital, jnp.arange(NOCC, dtype=jnp.int32))
```

```python
import functools

import jax
import jax.numpy as jnp
from jax import lax
from jax.experimental import pallas as pl
from jax.experimental.pallas import tpu as pltpu
from jax.sharding import PartitionSpec as P

CYCLE = 4
MESH = pl.DeviceIdType.MESH
NT = (((1,), (1,)), ((), ()))


def offset_of(slot):
    size = CYCLE + 1 - (slot + 1) // 2
    return 0 if slot == 0 else (size if slot % 2 else -size)


def pairs_kernel(
    aux_count, share, own_ref, occ_ref, vir_row_ref, vir_col_ref, out_ref,
    slots, own_t, vis_t, vir_pairs, amp, mix, acc, outgoing, incoming,
    send_sems, recv_sems, swap_sems,
):
    me = lax.axis_index("aux")
    core = lax.axis_index("ao")
    other = 1 - core
    block, _, nvir = own_ref.shape
    half = nvir // 2
    slot_count = 2 * CYCLE + 1

    barrier = pltpu.get_barrier_semaphore()
    for slot in range(1, slot_count):
        target = lax.rem(me + aux_count + offset_of(slot), aux_count)
        pl.semaphore_signal(barrier, inc=1, device_id=(target, core), device_id_type=MESH)
    pl.semaphore_signal(barrier, inc=1, device_id=(me, other), device_id_type=MESH)
    pl.semaphore_wait(barrier, slot_count)

    piece = own_ref.at[pl.ds(core * share, share)]
    sends = []
    for slot in range(1, slot_count):
        target = lax.rem(me + aux_count - offset_of(slot), aux_count)
        sends.append(
            pltpu.make_async_remote_copy(
                src_ref=piece,
                dst_ref=slots.at[slot],
                send_sem=send_sems.at[slot],
                recv_sem=recv_sems.at[slot],
                device_id=(target, core),
                device_id_type=MESH,
            )
        )
        sends[-1].start()
    pltpu.make_async_copy(piece, slots.at[0], recv_sems.at[0]).start()

    for i in range(block):
        own_t[i] = own_ref[i].T
    vir_pairs[...] = vir_col_ref[...] + vir_row_ref[...]
    acc[...] = jnp.zeros_like(acc)

    def visit(slot, carry):
        size = CYCLE + 1 - lax.div(slot + 1, 2)
        signed = jnp.where(lax.rem(slot, 2) == 1, size, -size)
        offset = jnp.where(slot == 0, 0, signed)
        owner = lax.rem(me + aux_count + offset, aux_count)
        pltpu.make_async_copy(slots.at[slot], slots.at[slot], recv_sems.at[slot]).wait()
        for s in range(share):
            pair_energy = occ_ref[owner * block + core * share + s]
            visitor = slots[slot, s]
            vis_t[...] = visitor.T
            for i in range(block):
                energy = occ_ref[me * block + i] + pair_energy
                for t in range(2):
                    rows = slice(t * half, (t + 1) * half)
                    direct = jnp.dot(own_t[i, rows], visitor, preferred_element_type=jnp.float32)
                    swapped = jnp.dot(vis_t[rows], own_ref[i], preferred_element_type=jnp.float32)
                    inverse = 1.0 / (energy - vir_pairs[rows])
                    amp[i, rows] = (direct * inverse).astype(jnp.bfloat16)
                    mix[i, rows] = ((2.0 * direct - swapped) * inverse).astype(jnp.bfloat16)
                acc[i] += lax.dot_general(amp[i], mix[i], NT, preferred_element_type=jnp.float32)
        return carry

    lax.fori_loop(0, slot_count, visit, 0)

    outgoing[...] = acc[:, pl.ds(pl.multiple_of(other * half, half), half)].astype(jnp.bfloat16)
    swap = pltpu.make_async_remote_copy(
        src_ref=outgoing,
        dst_ref=incoming,
        send_sem=swap_sems.at[0],
        recv_sem=swap_sems.at[1],
        device_id=(me, other),
        device_id_type=MESH,
    )
    swap.start()
    for send in sends:
        send.wait_send()
    swap.wait()
    kept = acc[:, pl.ds(pl.multiple_of(core * half, half), half)]
    out_ref[...] = kept + incoming[...].astype(jnp.float32)


def pair_densities(own_block, occ_energy, vir_energy, aux_count, share):
    block, naux, nvir = own_block.shape
    half = nvir // 2
    slot_count = 2 * CYCLE + 1
    vmem = pl.BlockSpec(memory_space=pltpu.VMEM)
    return pl.pallas_call(
        functools.partial(pairs_kernel, aux_count, share),
        out_shape=jax.ShapeDtypeStruct((block, half, nvir), jnp.float32),
        in_specs=[vmem, pl.BlockSpec(memory_space=pltpu.SMEM), vmem, vmem],
        out_specs=vmem,
        scratch_shapes=[
            pltpu.VMEM((slot_count, share, naux, nvir), jnp.bfloat16),
            pltpu.VMEM((block, nvir, naux), jnp.bfloat16),
            pltpu.VMEM((nvir, naux), jnp.bfloat16),
            pltpu.VMEM((nvir, nvir), jnp.float32),
            pltpu.VMEM((block, nvir, nvir), jnp.bfloat16),
            pltpu.VMEM((block, nvir, nvir), jnp.bfloat16),
            pltpu.VMEM((block, nvir, nvir), jnp.float32),
            pltpu.VMEM((block, half, nvir), jnp.bfloat16),
            pltpu.VMEM((block, half, nvir), jnp.bfloat16),
            pltpu.SemaphoreType.DMA((slot_count,)),
            pltpu.SemaphoreType.DMA((slot_count,)),
            pltpu.SemaphoreType.DMA((2,)),
        ],
        compiler_params=pltpu.CompilerParams(collective_id=0, has_side_effects=True, vmem_limit_bytes=48 * 2**20),
    )(own_block, occ_energy, vir_energy[None, :], vir_energy[:, None])


def shards(ints, occ_coef, vir_coef, occ_energy, vir_energy):
    core = lax.axis_index("ao")
    aux_count = lax.axis_size("aux")
    ao_count = lax.axis_size("ao")
    share = occ_coef.shape[1] // aux_count // ao_count
    half = vir_coef.shape[1] // ao_count
    half_ints = jnp.einsum(
        "qmn,ni->qmi", ints, occ_coef, preferred_element_type=jnp.float32
    ).astype(jnp.bfloat16)
    partial_sum = jnp.einsum("qmi,ma->qia", half_ints, vir_coef, preferred_element_type=jnp.float32)
    given = lax.dynamic_slice_in_dim(partial_sum, (1 - core) * half, half, 2).astype(jnp.bfloat16)
    taken = lax.ppermute(given, "ao", [(0, 1), (1, 0)])
    kept = lax.dynamic_slice_in_dim(partial_sum, core * half, half, 2)
    summed = (kept + taken.astype(jnp.float32)).astype(jnp.bfloat16)
    grouped = lax.all_to_all(summed, "aux", split_axis=1, concat_axis=0, tiled=True)
    own_block = lax.all_gather(grouped, "ao", axis=2, tiled=True)
    return pair_densities(
        jnp.swapaxes(own_block, 0, 1), occ_energy, vir_energy, aux_count, share
    )


def solution(mesh):
    return jax.shard_map(
        shards,
        mesh=mesh,
        in_specs=(P("aux", "ao", None), P(), P("ao", None), P(), P()),
        out_specs=P("aux", "ao", None),
        check_vma=False,
    )
```

```python
import functools

import jax
import jax.numpy as jnp
from jax import lax
from jax.experimental import pallas as pl
from jax.experimental.pallas import tpu as pltpu
from jax.sharding import PartitionSpec as P

CYCLE = 4
MESH = pl.DeviceIdType.MESH
NT = (((1,), (1,)), ((), ()))


def offset_of(slot):
    size = CYCLE + 1 - (slot + 1) // 2
    return 0 if slot == 0 else (size if slot % 2 else -size)


def pairs_kernel(
    aux_count, ao_count, share, slab_ref, occ_ref, vir_row_ref, vir_col_ref, out_ref,
    own_ref, slots, own_t, vis_t, vir_pairs, amp, mix, acc, outgoing, incoming,
    spread_sems, gather_sems, send_sems, recv_sems, swap_sems,
):
    me = lax.axis_index("aux")
    core = lax.axis_index("ao")
    other = 1 - core
    block, _, nvir = own_ref.shape
    half = nvir // 2
    slot_count = 2 * CYCLE + 1
    total = aux_count * ao_count
    rank = me * ao_count + core
    slab_rows = slab_ref.shape[1]
    slab_columns = slab_ref.shape[2]

    def place_of(number):
        aux, ao = lax.div(number, ao_count), lax.rem(number, ao_count)
        rows = pl.ds(pl.multiple_of(aux * slab_rows, slab_rows), slab_rows)
        columns = pl.ds(pl.multiple_of(ao * slab_columns, slab_columns), slab_columns)
        return own_ref.at[:, rows, columns]

    def spread(step):
        number = lax.rem(rank + step, total)
        aux, ao = lax.div(number, ao_count), lax.rem(number, ao_count)
        return pltpu.make_async_remote_copy(
            src_ref=slab_ref.at[pl.ds(aux * block, block)],
            dst_ref=place_of(rank),
            send_sem=spread_sems.at[step],
            recv_sem=gather_sems.at[step],
            device_id=(aux, ao),
            device_id_type=MESH,
        )

    barrier = pltpu.get_barrier_semaphore()

    def greet(step, carry):
        number = lax.rem(rank + step, total)
        target = (lax.div(number, ao_count), lax.rem(number, ao_count))
        pl.semaphore_signal(barrier, inc=1, device_id=target, device_id_type=MESH)
        return carry

    def start_spread(step, carry):
        spread(step).start()
        return carry

    def end_spread(step, carry):
        spread(step).wait_send()
        return carry

    def gather(step, carry):
        place = place_of(lax.rem(rank + total - step, total))
        pltpu.make_async_copy(place, place, gather_sems.at[step]).wait()
        return carry

    lax.fori_loop(1, total, greet, 0)
    vir_pairs[...] = vir_col_ref[...] + vir_row_ref[...]
    acc[...] = jnp.zeros_like(acc)
    pl.semaphore_wait(barrier, total - 1)
    lax.fori_loop(1, total, start_spread, 0)
    pltpu.make_async_copy(
        slab_ref.at[pl.ds(me * block, block)], place_of(rank), gather_sems.at[0]
    ).start()
    lax.fori_loop(0, total, gather, 0)

    piece = own_ref.at[pl.ds(core * share, share)]
    sends = []
    for slot in range(1, slot_count):
        target = lax.rem(me + aux_count - offset_of(slot), aux_count)
        sends.append(
            pltpu.make_async_remote_copy(
                src_ref=piece,
                dst_ref=slots.at[slot],
                send_sem=send_sems.at[slot],
                recv_sem=recv_sems.at[slot],
                device_id=(target, core),
                device_id_type=MESH,
            )
        )
        sends[-1].start()
    pltpu.make_async_copy(piece, slots.at[0], recv_sems.at[0]).start()

    for i in range(block):
        own_t[i] = own_ref[i].T

    def visit(slot, carry):
        size = CYCLE + 1 - lax.div(slot + 1, 2)
        signed = jnp.where(lax.rem(slot, 2) == 1, size, -size)
        offset = jnp.where(slot == 0, 0, signed)
        owner = lax.rem(me + aux_count + offset, aux_count)
        pltpu.make_async_copy(slots.at[slot], slots.at[slot], recv_sems.at[slot]).wait()
        for s in range(share):
            pair_energy = occ_ref[owner * block + core * share + s]
            visitor = slots[slot, s]
            vis_t[...] = visitor.T
            for i in range(block):
                energy = occ_ref[me * block + i] + pair_energy
                for t in range(2):
                    rows = slice(t * half, (t + 1) * half)
                    direct = jnp.dot(own_t[i, rows], visitor, preferred_element_type=jnp.float32)
                    swapped = jnp.dot(vis_t[rows], own_ref[i], preferred_element_type=jnp.float32)
                    inverse = 1.0 / (energy - vir_pairs[rows])
                    amp[i, rows] = (direct * inverse).astype(jnp.bfloat16)
                    mix[i, rows] = ((2.0 * direct - swapped) * inverse).astype(jnp.bfloat16)
                acc[i] += lax.dot_general(amp[i], mix[i], NT, preferred_element_type=jnp.float32)
        return carry

    lax.fori_loop(0, slot_count, visit, 0)

    outgoing[...] = acc[:, pl.ds(pl.multiple_of(other * half, half), half)].astype(jnp.bfloat16)
    swap = pltpu.make_async_remote_copy(
        src_ref=outgoing,
        dst_ref=incoming,
        send_sem=swap_sems.at[0],
        recv_sem=swap_sems.at[1],
        device_id=(me, other),
        device_id_type=MESH,
    )
    swap.start()
    for send in sends:
        send.wait_send()
    lax.fori_loop(1, total, end_spread, 0)
    swap.wait()
    kept = acc[:, pl.ds(pl.multiple_of(core * half, half), half)]
    out_ref[...] = kept + incoming[...].astype(jnp.float32)


def pair_densities(slab, occ_energy, vir_energy, aux_count, ao_count, share):
    block = slab.shape[0] // aux_count
    naux = slab.shape[1] * aux_count
    nvir = slab.shape[2] * ao_count
    total = aux_count * ao_count
    half = nvir // 2
    slot_count = 2 * CYCLE + 1
    vmem = pl.BlockSpec(memory_space=pltpu.VMEM)
    return pl.pallas_call(
        functools.partial(pairs_kernel, aux_count, ao_count, share),
        out_shape=jax.ShapeDtypeStruct((block, half, nvir), jnp.float32),
        in_specs=[vmem, pl.BlockSpec(memory_space=pltpu.SMEM), vmem, vmem],
        out_specs=vmem,
        scratch_shapes=[
            pltpu.VMEM((block, naux, nvir), jnp.bfloat16),
            pltpu.VMEM((slot_count, share, naux, nvir), jnp.bfloat16),
            pltpu.VMEM((block, nvir, naux), jnp.bfloat16),
            pltpu.VMEM((nvir, naux), jnp.bfloat16),
            pltpu.VMEM((nvir, nvir), jnp.float32),
            pltpu.VMEM((block, nvir, nvir), jnp.bfloat16),
            pltpu.VMEM((block, nvir, nvir), jnp.bfloat16),
            pltpu.VMEM((block, nvir, nvir), jnp.float32),
            pltpu.VMEM((block, half, nvir), jnp.bfloat16),
            pltpu.VMEM((block, half, nvir), jnp.bfloat16),
            pltpu.SemaphoreType.DMA((total,)),
            pltpu.SemaphoreType.DMA((total,)),
            pltpu.SemaphoreType.DMA((slot_count,)),
            pltpu.SemaphoreType.DMA((slot_count,)),
            pltpu.SemaphoreType.DMA((2,)),
        ],
        compiler_params=pltpu.CompilerParams(collective_id=0, has_side_effects=True, vmem_limit_bytes=48 * 2**20),
    )(slab, occ_energy, vir_energy[None, :], vir_energy[:, None])


def shards(ints, occ_coef, vir_coef, occ_energy, vir_energy):
    core = lax.axis_index("ao")
    aux_count = lax.axis_size("aux")
    ao_count = lax.axis_size("ao")
    share = occ_coef.shape[1] // aux_count // ao_count
    half = vir_coef.shape[1] // ao_count
    half_ints = jnp.einsum(
        "qmn,ni->qmi", ints, occ_coef, preferred_element_type=jnp.float32
    ).astype(jnp.bfloat16)
    partial_sum = jnp.einsum("qmi,ma->qia", half_ints, vir_coef, preferred_element_type=jnp.float32)
    given = lax.dynamic_slice_in_dim(partial_sum, (1 - core) * half, half, 2).astype(jnp.bfloat16)
    taken = lax.ppermute(given, "ao", [(0, 1), (1, 0)])
    kept = lax.dynamic_slice_in_dim(partial_sum, core * half, half, 2)
    summed = (kept + taken.astype(jnp.float32)).astype(jnp.bfloat16)
    return pair_densities(
        jnp.swapaxes(summed, 0, 1), occ_energy, vir_energy, aux_count, ao_count, share
    )


def solution(mesh):
    return jax.shard_map(
        shards,
        mesh=mesh,
        in_specs=(P("aux", "ao", None), P(), P("ao", None), P(), P()),
        out_specs=P("aux", "ao", None),
        check_vma=False,
    )
```
